32 devices in a mesh: grp: 2 (over y), tm: 16 (over z, x, core).
Axes of the slice: x: 2, y: 2, z: 4, core: 2. Of those that a mesh axis runs over, the one named last changes fastest.
Arguments:
- traces: float32 [2048, 16384], P('grp', 'tm'), parts along dimension 0, may hold values from -6 to 6
- templates: float32 [64, 8192], P('tm'), may hold values from -6 to 6
- moveouts: int32 [2048], P('grp'), parts along dimension 0, may hold values from 0 to 2047
- masks: int32 [64, 2048], P(None, 'grp'), parts along dimension 1, may hold values 0 or 1
Outputs:
- detection: float32 [64, 16384], P('tm', 'grp'), parts along dimension 1
The draws below stay inside these ranges and needn't reach their ends.
There are 2 independent parts, one for each index of `grp`. The reference program is written for one: setup_inputs(seed, part) draws one part's arguments, and reference() takes and returns one part's arrays. A program takes and returns all parts, laid end to end along the dimension named above; an argument that names none is the same for every part. Nothing has to cross between parts.
All inputs are finite; a program needn't handle non-finite values.
Results may differ from the reference program's by a relative error of at most 0.000073.
Values sent between devices are 32-bit elements; how exact they have to be, the bound alone decides.
A program may use at most 64 MiB of HBM per device.

```python
import math
import jax
import jax.numpy as jnp
from jax import lax

C = 1024
L = 8192
NF = 16384
K = 64


def with_ends(drawn, key, least, top_value):
    index_at = [jax.random.randint(jax.random.fold_in(key, axis), (), 0, length) for axis, length in enumerate(drawn.shape)]
    main_axis = drawn.shape.index(max(drawn.shape))
    beside = index_at[:main_axis] + [(index_at[main_axis] + 1) % drawn.shape[main_axis]] + index_at[main_axis + 1:]
    return drawn.at[tuple(index_at)].set(least).at[tuple(beside)].set(top_value)


def block_scale(stream_key, dims, shards, low, top_value):
    def one(position, blocks):
        steps = jax.random.uniform(jax.random.fold_in(jax.random.fold_in(stream_key, 6), position), (blocks,), jnp.float32, low / len(shards), top_value / len(shards))
        return jnp.repeat(jnp.exp(steps), dims[position] // blocks).reshape((-1,) + (1,) * (len(dims) - position - 1))

    factor_of = one(*shards[0])
    for cut in shards[1:]:
        factor_of = factor_of * one(*cut)
    return factor_of


def gaussian(rng, dims, deviation, limit, split=(), kind=jnp.bfloat16):
    array = deviation * jax.random.normal(rng, dims, jnp.float32)
    if split:
        array = array * block_scale(rng, dims, split, -0.22, 0.18)
    return jnp.clip(array, -limit, limit).astype(kind)


def setup_inputs(seed: int = 0, part: int = 0) -> dict:
    arg_keys = jax.random.split(jax.random.key(seed), 5)
    part_keys = jax.random.split(jax.random.fold_in(arg_keys[4], part), 5)
    return {
        "traces": gaussian(part_keys[0], (C, NF), 1.0, 6.0, ((1, 16),), jnp.float32),
        "templates": gaussian(arg_keys[1], (K, L), 1.0, 6.0, ((0, 16),), jnp.float32),
        "moveouts": with_ends(jax.random.randint(part_keys[2], (C,), 0, NF // 8), jax.random.fold_in(part_keys[2], 1), 0, (NF // 8) - 1).astype(jnp.int32),
        "masks": with_ends((jax.random.randint(part_keys[3], (K, C), 0, 4) < 3).astype(jnp.int32), jax.random.fold_in(part_keys[3], 1), 0, 1),
    }


def reference(traces, templates, moveouts, masks):
    length = traces.shape[1]
    spectra = jnp.fft.fft(traces, axis=1)
    freqs = jnp.arange(length).astype(jnp.int32)
    angle = 2.0 * math.pi / length * (moveouts.astype(jnp.int32)[:, None] * freqs[None, :] % length).astype(jnp.float32)
    moved = spectra * (jnp.cos(angle) + 1j * jnp.sin(angle))
    mask_float = masks.astype(jnp.float32)
    stacked_re = jnp.dot(mask_float, jnp.real(moved), precision=lax.Precision.HIGHEST, preferred_element_type=jnp.float32)
    stacked_im = jnp.dot(mask_float, jnp.imag(moved), precision=lax.Precision.HIGHEST, preferred_element_type=jnp.float32)
    template_spectra = jnp.fft.fft(templates, n=length, axis=1)
    product = (stacked_re + 1j * stacked_im) * jnp.conj(template_spectra)
    correlation = jnp.real(jnp.fft.ifft(product, axis=1))[:, :templates.shape[1]]
    energy = jnp.sqrt(lax.optimization_barrier(jnp.sum(templates * templates, axis=1)) + 1e-06)
    return correlation / (math.sqrt(traces.shape[0]) * energy[:, None])
```

```python
import functools
import math

import jax
import jax.numpy as jnp
import numpy as np
from jax import lax
from jax.experimental import pallas as pl
from jax.experimental.pallas import tpu as pltpu
from jax.sharding import PartitionSpec as P

f32, bf16 = jnp.float32, jnp.bfloat16
LANES = 128
REACH = 2048


def split(value):
    high = value.astype(bf16)
    return high, (value - high.astype(f32)).astype(bf16)


def split_table(table):
    high = table.astype(jnp.bfloat16)
    return high, (table - high.astype(np.float64)).astype(jnp.bfloat16)


def stack_kernel(owners, moveout_ref, mask_ref, traces_ref, out_ref, late, terms, total):
    step = pl.program_id(0)
    channels, width = traces_ref.shape
    blocks = width // LANES
    window = blocks + REACH // LANES
    for part in range(channels // LANES):
        row = (REACH - 1) - moveout_ref[:, part * LANES : (part + 1) * LANES]
        late[part * LANES : (part + 1) * LANES, :] = jnp.broadcast_to(row, (LANES, LANES)).T

    rows = 16

    def shift(group, _):
        here = pl.ds(pl.multiple_of(group * rows, rows), rows)
        delay = late[here, :]
        lane = lax.broadcasted_iota(jnp.int32, (rows, LANES), 1)
        inner = (delay & (LANES - 1)) + 1
        index = (lane - inner) & (LANES - 1)
        keep = lane >= inner
        turned = [
            jnp.take_along_axis(
                traces_ref[here, b * LANES : (b + 1) * LANES], index, axis=1, mode="promise_in_bounds"
            )
            for b in range(blocks)
        ]
        zero = jnp.zeros((rows, LANES), f32)
        moved = [
            jnp.where(keep, turned[b] if b < blocks else zero, turned[b - 1] if b > 0 else zero)
            for b in range(blocks + 1)
        ]
        hop = 1
        while hop < REACH // LANES:
            chosen = ((delay // LANES) & hop) != 0
            moved = [
                jnp.where(
                    chosen,
                    moved[b - hop] if b >= hop else zero,
                    moved[b] if b < len(moved) else zero,
                )
                for b in range(len(moved) + hop)
            ]
            hop *= 2
        for b in range(window):
            high, low = split(moved[b])
            terms[here, b * LANES : (b + 1) * LANES] = high
            terms[pl.ds(pl.multiple_of(channels + group * rows, rows), rows), b * LANES : (b + 1) * LANES] = low
        return 0

    lax.fori_loop(0, channels // rows, shift, 0)
    mask = mask_ref[...].astype(f32).astype(bf16)
    added = jnp.dot(
        jnp.concatenate([mask, mask], axis=1), terms[...], preferred_element_type=f32
    )

    @pl.when(step == 0)
    def _():
        total[...] = added

    @pl.when(step > 0)
    def _():
        total[...] += added

    @pl.when(step == pl.num_programs(0) - 1)
    def _():
        each = mask_ref.shape[0] // owners
        for owner in range(owners):
            for b in range(window):
                out_ref[owner, b * each : (b + 1) * each, :] = total[
                    owner * each : (owner + 1) * each, b * LANES : (b + 1) * LANES
                ]


def exchange_kernel(devices, part_ref, out_ref, send_sem, recv_sem, own_sem):
    me = lax.axis_index("tm")

    def greet(i, _):
        pl.semaphore_signal(
            barrier, inc=1, device_id={"tm": lax.rem(me + i, devices)}, device_id_type=pl.DeviceIdType.MESH
        )
        return 0

    barrier = pltpu.get_barrier_semaphore()
    lax.fori_loop(1, devices, greet, 0)
    pl.semaphore_wait(barrier, devices - 1)

    def copy(i):
        target = lax.rem(me + i, devices)
        return pltpu.make_async_remote_copy(
            src_ref=part_ref.at[target],
            dst_ref=out_ref.at[me],
            send_sem=send_sem.at[i],
            recv_sem=recv_sem.at[i],
            device_id={"tm": target},
            device_id_type=pl.DeviceIdType.MESH,
        )

    def send(i, _):
        copy(i).start()
        return 0

    def finish(i, _):
        copy(i).wait()
        return 0

    lax.fori_loop(1, devices, send, 0)
    own = pltpu.make_async_copy(part_ref.at[me], out_ref.at[me], own_sem)
    own.start()
    own.wait()
    lax.fori_loop(1, devices, finish, 0)


def three(left_high, left_low, right_high, right_low):
    left = jnp.concatenate([left_high, left_low, left_high], axis=1)
    right = jnp.concatenate([right_high, right_high, right_low], axis=0)
    return jnp.dot(left, right, preferred_element_type=f32)


def correlate_kernel(
    channels, parts_ref, templates_ref, first_ref, forward_ref, back_ref, last_ref, twiddle_ref, out_ref, series, tail
):
    devices = parts_ref.shape[0]
    each, lags = templates_ref.shape
    outer = first_ref.shape[1] // 3
    length = outer * LANES
    local = outer // devices
    window = local + REACH // LANES
    for device in range(devices):
        for b in range(0, window, local):
            count = min(local, window - b)
            block = (device * local + b - REACH // LANES) % outer
            here = slice(block * each, (block + count) * each)
            added = parts_ref[device, b * each : (b + count) * each, :]
            if b == 0 and device == 0:
                series[0 : outer * each, :] = jnp.zeros((outer * each, LANES), f32)
            series[here, :] = series[here, :] + added
    base = outer * each
    values = templates_ref[...]
    for b in range(lags // LANES):
        series[base + b * each : base + (b + 1) * each, :] = values[:, b * LANES : (b + 1) * LANES]
    series[base + lags // LANES * each :, :] = jnp.zeros(((outer - lags // LANES) * each, LANES), f32)
    energy = jnp.sqrt(jnp.sum(values * values, axis=1, keepdims=True) + 1e-06)
    factor = 1.0 / (length * math.sqrt(channels) * energy)

    columns = [series[pl.ds(half * base + k, outer, stride=each), :] for half in range(2) for k in range(each)]
    high, low = split(jnp.concatenate(columns, axis=1))
    first = jnp.dot(first_ref[...], jnp.concatenate([high, high, low], axis=0), preferred_element_type=f32)
    cosine, sine = twiddle_ref[0], twiddle_ref[1]
    spectra = []
    for r in range(2 * each):
        re = first[:outer, r * LANES : (r + 1) * LANES]
        im = first[outer:, r * LANES : (r + 1) * LANES]
        spectra.append(jnp.concatenate([re * cosine + im * sine, im * cosine - re * sine], axis=1))
    high, low = split(jnp.concatenate(spectra, axis=0))
    full = jnp.dot(jnp.concatenate([high, low, high], axis=1), forward_ref[...], preferred_element_type=f32)
    stack, templ = full[: each * outer], full[each * outer :]
    stack_re, stack_im = stack[:, :LANES], stack[:, LANES:]
    templ_re, templ_im = templ[:, :LANES], templ[:, LANES:]
    product = jnp.concatenate(
        [stack_re * templ_re + stack_im * templ_im, stack_im * templ_re - stack_re * templ_im], axis=1
    )
    high, low = split(product)
    back = jnp.dot(jnp.concatenate([high, low, high], axis=1), back_ref[...], preferred_element_type=f32)
    turned = []
    for k in range(each):
        re = back[k * outer : (k + 1) * outer, :LANES]
        im = back[k * outer : (k + 1) * outer, LANES:]
        turned.append(jnp.concatenate([re * cosine - im * sine, re * sine + im * cosine], axis=0))
    high, low = split(jnp.concatenate(turned, axis=1))
    final = jnp.dot(last_ref[...], jnp.concatenate([high, high, low], axis=0), preferred_element_type=f32)
    count = lags // LANES
    for k in range(each):
        tail[pl.ds(k, count, stride=each), :] = final[:, k * LANES : (k + 1) * LANES]
    for b in range(count):
        out_ref[:, b * LANES : (b + 1) * LANES] = tail[b * each : (b + 1) * each, :] * factor


def tables(length, lags):
    outer = length // LANES
    turn = 2.0 * math.pi
    ramp = np.arange(outer)[:, None] * np.arange(outer)[None, :] % outer * (turn / outer)
    wide = np.arange(LANES)[:, None] * np.arange(LANES)[None, :] % LANES * (turn / LANES)
    twist = np.arange(outer)[:, None] * np.arange(LANES)[None, :] % length * (turn / length)
    first = split_table(np.concatenate([np.cos(ramp), -np.sin(ramp)], axis=0))
    cosine, sine = np.cos(wide), np.sin(wide)
    forward = split_table(np.block([[cosine, -sine], [sine, cosine]]))
    back = split_table(np.block([[cosine, sine], [-sine, cosine]]))
    shown = ramp[: lags // LANES]
    last = split_table(np.concatenate([np.cos(shown), -np.sin(shown)], axis=1))
    return (
        np.concatenate([first[0], first[1], first[0]], axis=1),
        np.concatenate([forward[0], forward[0], forward[1]], axis=0),
        np.concatenate([back[0], back[0], back[1]], axis=0),
        np.concatenate([last[0], last[1], last[0]], axis=1),
        np.stack([np.cos(twist), np.sin(twist)]).astype(np.float32),
    )


def on_device(devices, traces, templates, moveouts, masks):
    channels, width = traces.shape
    count = masks.shape[0]
    each, lags = templates.shape
    length = width * devices
    window = width // LANES + REACH // LANES
    depth = math.gcd(channels, 256)
    vmem = pl.BlockSpec(memory_space=pltpu.VMEM)
    partial = pl.pallas_call(
        functools.partial(stack_kernel, devices),
        grid=(channels // depth,),
        in_specs=[
            pl.BlockSpec((1, depth), lambda i: (0, i)),
            pl.BlockSpec((count, depth), lambda i: (0, i)),
            pl.BlockSpec((depth, width), lambda i: (i, 0)),
        ],
        out_specs=pl.BlockSpec((devices, window * each, LANES), lambda i: (0, 0, 0)),
        out_shape=jax.ShapeDtypeStruct((devices, window * each, LANES), f32),
        scratch_shapes=[
            pltpu.VMEM((depth, LANES), jnp.int32),
            pltpu.VMEM((2 * depth, window * LANES), bf16),
            pltpu.VMEM((count, window * LANES), f32),
        ],
        name="stack",
    )(moveouts[None, :], masks, traces)
    parts = pl.pallas_call(
        functools.partial(exchange_kernel, devices),
        in_specs=[vmem],
        out_specs=vmem,
        out_shape=jax.ShapeDtypeStruct(partial.shape, f32),
        scratch_shapes=[
            pltpu.SemaphoreType.DMA((devices,)),
            pltpu.SemaphoreType.DMA((devices,)),
            pltpu.SemaphoreType.DMA,
        ],
        compiler_params=pltpu.CompilerParams(collective_id=0, has_side_effects=True),
        name="exchange",
    )(partial)
    outer = length // LANES
    return pl.pallas_call(
        functools.partial(correlate_kernel, channels),
        in_specs=[vmem] * 7,
        out_specs=vmem,
        out_shape=jax.ShapeDtypeStruct((each, lags), f32),
        scratch_shapes=[
            pltpu.VMEM((2 * outer * each, LANES), f32),
            pltpu.VMEM((lags // LANES * each, LANES), f32),
        ],
        name="correlate",
    )(parts, templates, *[jnp.asarray(table) for table in tables(length, lags)])


def solution(mesh):
    return jax.shard_map(
        functools.partial(on_device, mesh.shape["tm"]),
        mesh=mesh,
        in_specs=(P("grp", "tm"), P("tm", None), P("grp"), P(None, "grp")),
        out_specs=P("tm", "grp"),
        check_vma=False,
    )
```

```python
import functools
import math

import jax
import jax.numpy as jnp
import numpy as np
from jax import lax
from jax.experimental import pallas as pl
from jax.experimental.pallas import tpu as pltpu
from jax.sharding import PartitionSpec as P

f32, bf16 = jnp.float32, jnp.bfloat16
LANES = 128
REACH = 2048


def split(value):
    high = value.astype(bf16)
    return high, (value - high.astype(f32)).astype(bf16)


def split_table(table):
    high = table.astype(jnp.bfloat16)
    return high, (table - high.astype(np.float64)).astype(jnp.bfloat16)


def transform(rows, first_ref, forward_ref, cosine, sine):
    outer = cosine.shape[0]
    high, low = split(jnp.concatenate(rows, axis=1))
    first = jnp.dot(first_ref[...], jnp.concatenate([high, high, low], axis=0), preferred_element_type=f32)
    turned = []
    for r in range(len(rows)):
        re = first[:outer, r * LANES : (r + 1) * LANES]
        im = first[outer:, r * LANES : (r + 1) * LANES]
        turned.append(jnp.concatenate([re * cosine + im * sine, im * cosine - re * sine], axis=1))
    high, low = split(jnp.concatenate(turned, axis=0))
    return jnp.dot(jnp.concatenate([high, low, high], axis=1), forward_ref[...], preferred_element_type=f32)


def shift(traces_ref, late, terms, base, group, channels):
    rows = 16
    blocks = traces_ref.shape[1] // LANES
    window = blocks + REACH // LANES
    here = pl.ds(pl.multiple_of(group * rows, rows), rows)
    delay = late[here, :]
    lane = lax.broadcasted_iota(jnp.int32, (rows, LANES), 1)
    inner = (delay & (LANES - 1)) + 1
    index = (lane - inner) & (LANES - 1)
    keep = lane >= inner
    turned = [
        jnp.take_along_axis(
            traces_ref[here, b * LANES : (b + 1) * LANES], index, axis=1, mode="promise_in_bounds"
        )
        for b in range(blocks)
    ]
    zero = jnp.zeros((rows, LANES), f32)
    moved = [
        jnp.where(keep, turned[b] if b < blocks else zero, turned[b - 1] if b > 0 else zero)
        for b in range(blocks + 1)
    ]
    hop = 1
    while hop < REACH // LANES:
        chosen = ((delay // LANES) & hop) != 0
        moved = [
            jnp.where(
                chosen,
                moved[b - hop] if b >= hop else zero,
                moved[b] if b < len(moved) else zero,
            )
            for b in range(len(moved) + hop)
        ]
        hop *= 2
    for b in range(window):
        high, low = split(moved[b])
        column = slice(b * LANES, (b + 1) * LANES)
        terms[pl.ds(pl.multiple_of(base + group * rows, rows), rows), column] = high
        terms[pl.ds(pl.multiple_of(channels + base + group * rows, rows), rows), column] = low


def kernel(
    devices,
    channels,
    moveout_ref,
    traces_ref,
    mask_hbm,
    template_hbm,
    first_hbm,
    forward_hbm,
    back_hbm,
    last_hbm,
    twiddle_hbm,
    out_ref,
    mask_ref,
    template_ref,
    first_ref,
    forward_ref,
    back_ref,
    last_ref,
    twiddle_ref,
    late,
    terms,
    part,
    arrived,
    merged,
    joined,
    series,
    tail,
    load_sem,
    pair_send,
    pair_recv,
    send_sem,
    recv_sem,
):
    step = pl.program_id(0)
    steps = pl.num_programs(0)
    depth, width = traces_ref.shape
    each, lags = template_ref.shape
    pairs = devices // 2
    me = lax.axis_index("tm")
    core = lax.rem(me, 2)
    pair = me // 2
    partner = me + 1 - 2 * core
    blocks = width // LANES
    window = blocks + REACH // LANES
    outer = devices * blocks
    loads = [
        pltpu.make_async_copy(source, target, load_sem.at[i])
        for i, (source, target) in enumerate(
            (
                (mask_hbm, mask_ref),
                (template_hbm, template_ref),
                (first_hbm, first_ref),
                (forward_hbm, forward_ref),
                (twiddle_hbm, twiddle_ref),
                (back_hbm, back_ref),
                (last_hbm, last_ref),
            )
        )
    ]
    barrier = pltpu.get_barrier_semaphore()

    @pl.when(step == 0)
    def _():
        for load in loads:
            load.start()

        def greet(i, _):
            target = 2 * lax.rem(pair + i, pairs) + core
            pl.semaphore_signal(barrier, inc=1, device_id={"tm": target}, device_id_type=pl.DeviceIdType.MESH)
            return 0

        pl.semaphore_signal(barrier, inc=1, device_id={"tm": partner}, device_id_type=pl.DeviceIdType.MESH)
        lax.fori_loop(1, pairs, greet, 0)

    for piece in range(depth // LANES):
        row = (REACH - 1) - moveout_ref[:, piece * LANES : (piece + 1) * LANES]
        late[piece * LANES : (piece + 1) * LANES, :] = jnp.broadcast_to(row, (LANES, LANES)).T

    def group_pair(i, _):
        for k in range(2):
            shift(traces_ref, late, terms, step * depth, 2 * i + k, channels)
        return 0

    lax.fori_loop(0, depth // 32, group_pair, 0)

    def far(k):
        near = (k + 1) // 2
        return lax.rem(pair + pairs // 2 + near * (1 - 2 * lax.rem(k, 2)), pairs)

    def to_partner(g):
        return pltpu.make_async_remote_copy(
            src_ref=part.at[1 - core, g],
            dst_ref=arrived.at[g],
            send_sem=pair_send.at[g],
            recv_sem=pair_recv.at[g],
            device_id={"tm": partner},
            device_id_type=pl.DeviceIdType.MESH,
        )

    def to_owner(k):
        g = far(k)
        return pltpu.make_async_remote_copy(
            src_ref=merged.at[g],
            dst_ref=joined.at[pair],
            send_sem=send_sem.at[k],
            recv_sem=recv_sem.at[k],
            device_id={"tm": 2 * g + core},
            device_id_type=pl.DeviceIdType.MESH,
        )

    @pl.when(step == steps - 1)
    def _():
        loads[0].wait()
        mask = mask_ref[...].astype(f32).astype(bf16)
        double = jnp.concatenate([mask, mask], axis=1)
        span = 2 if window % 2 == 0 else 1
        for b in range(0, window, span):
            added = jnp.dot(double, terms[:, b * LANES : (b + span) * LANES], preferred_element_type=f32)
            for owner in range(devices):
                part[owner % 2, owner // 2, b * each : (b + span) * each, :] = jnp.concatenate(
                    [
                        added[owner * each : (owner + 1) * each, j * LANES : (j + 1) * LANES]
                        for j in range(span)
                    ],
                    axis=0,
                )
        pl.semaphore_wait(barrier, pairs)

        def first_send(k, _):
            to_partner(far(k)).start()
            return 0

        lax.fori_loop(0, pairs - 1, first_send, 0)
        to_partner(pair).start()
        rows, more = window * each, blocks * each

        def merge(g):
            to_partner(g).wait_recv()
            own, other = part[core, g], arrived[g]
            early = jnp.where(core == 0, own, other)
            later = jnp.where(core == 0, other, own)
            middle = early[more:] + later[: rows - more]
            return early[:more], middle, later[rows - more :]

        def second_send(k, _):
            g = far(k)
            begin, middle, end = merge(g)
            merged[g, 0:more] = begin
            merged[g, more:rows] = middle
            merged[g, rows : rows + more] = end
            to_owner(k).start()
            return 0

        lax.fori_loop(0, pairs - 1, second_send, 0)
        begin, middle, end = merge(pair)
        joined[pair, 0:more] = begin
        joined[pair, more:rows] = middle
        joined[pair, rows : rows + more] = end

        for load in loads[1:]:
            load.wait()
        cosine, sine = twiddle_ref[0], twiddle_ref[1]
        values = template_ref[...]
        count = lags // LANES
        for b in range(count):
            series[b * each : (b + 1) * each, :] = values[:, b * LANES : (b + 1) * LANES]
        series[count * each :, :] = jnp.zeros(((outer - count) * each, LANES), f32)
        energy = jnp.sqrt(jnp.sum(values * values, axis=1, keepdims=True) + 1e-06)
        factor = 1.0 / (outer * LANES * math.sqrt(channels) * energy)

        def columns():
            return [series[pl.ds(k, outer, stride=each), :] for k in range(each)]

        templ = transform(columns(), first_ref, forward_ref, cosine, sine)

        def finish(k, _):
            to_owner(k).wait()
            return 0

        lax.fori_loop(0, pairs - 1, finish, 0)

        def leave(g, _):
            to_partner(g).wait_send()
            return 0

        lax.fori_loop(0, pairs, leave, 0)
        series[...] = jnp.zeros(series.shape, f32)
        local = 2 * blocks
        wide = window + blocks
        for source in range(pairs):
            for b in range(0, wide, local):
                taken = min(local, wide - b)
                block = (source * local + b - REACH // LANES) % outer
                here = slice(block * each, (block + taken) * each)
                series[here, :] = series[here, :] + joined[source, b * each : (b + taken) * each, :]
        stack = transform(columns(), first_ref, forward_ref, cosine, sine)
        stack_re, stack_im = stack[:, :LANES], stack[:, LANES:]
        templ_re, templ_im = templ[:, :LANES], templ[:, LANES:]
        product = jnp.concatenate(
            [stack_re * templ_re + stack_im * templ_im, stack_im * templ_re - stack_re * templ_im], axis=1
        )
        high, low = split(product)
        back = jnp.dot(jnp.concatenate([high, low, high], axis=1), back_ref[...], preferred_element_type=f32)
        turned = []
        for k in range(each):
            re = back[k * outer : (k + 1) * outer, :LANES]
            im = back[k * outer : (k + 1) * outer, LANES:]
            turned.append(jnp.concatenate([re * cosine - im * sine, re * sine + im * cosine], axis=0))
        high, low = split(jnp.concatenate(turned, axis=1))
        final = jnp.dot(last_ref[...], jnp.concatenate([high, high, low], axis=0), preferred_element_type=f32)
        for k in range(each):
            tail[pl.ds(k, count, stride=each), :] = final[:, k * LANES : (k + 1) * LANES]
        for b in range(count):
            out_ref[:, b * LANES : (b + 1) * LANES] = tail[b * each : (b + 1) * each, :] * factor


def tables(length, lags):
    outer = length // LANES
    turn = 2.0 * math.pi
    ramp = np.arange(outer)[:, None] * np.arange(outer)[None, :] % outer * (turn / outer)
    wide = np.arange(LANES)[:, None] * np.arange(LANES)[None, :] % LANES * (turn / LANES)
    twist = np.arange(outer)[:, None] * np.arange(LANES)[None, :] % length * (turn / length)
    first = split_table(np.concatenate([np.cos(ramp), -np.sin(ramp)], axis=0))
    cosine, sine = np.cos(wide), np.sin(wide)
    forward = split_table(np.block([[cosine, -sine], [sine, cosine]]))
    back = split_table(np.block([[cosine, sine], [-sine, cosine]]))
    shown = ramp[: lags // LANES]
    last = split_table(np.concatenate([np.cos(shown), -np.sin(shown)], axis=1))
    return (
        np.concatenate([first[0], first[1], first[0]], axis=1),
        np.concatenate([forward[0], forward[0], forward[1]], axis=0),
        np.concatenate([back[0], back[0], back[1]], axis=0),
        np.concatenate([last[0], last[1], last[0]], axis=1),
        np.stack([np.cos(twist), np.sin(twist)]).astype(np.float32),
    )


def on_device(devices, traces, templates, moveouts, masks):
    channels, width = traces.shape
    each, lags = templates.shape
    blocks = width // LANES
    outer = devices * blocks
    window = blocks + REACH // LANES
    depth = math.gcd(channels, 256)
    pairs = devices // 2
    loaded = [masks, templates, *[jnp.asarray(table) for table in tables(outer * LANES, lags)]]
    wide = (window + blocks) * each
    return pl.pallas_call(
        functools.partial(kernel, devices, channels),
        grid=(channels // depth,),
        in_specs=[
            pl.BlockSpec((1, depth), lambda i: (0, i)),
            pl.BlockSpec((depth, width), lambda i: (i, 0)),
            *[pl.BlockSpec(memory_space=pl.ANY) for _ in loaded],
        ],
        out_specs=pl.BlockSpec((each, lags), lambda i: (0, 0)),
        out_shape=jax.ShapeDtypeStruct((each, lags), f32),
        scratch_shapes=[
            *[pltpu.VMEM(value.shape, value.dtype) for value in loaded],
            pltpu.VMEM((depth, LANES), jnp.int32),
            pltpu.VMEM((2 * channels, window * LANES), bf16),
            pltpu.VMEM((2, pairs, window * each, LANES), f32),
            pltpu.VMEM((pairs, window * each, LANES), f32),
            pltpu.VMEM((pairs, wide, LANES), f32),
            pltpu.VMEM((pairs, wide, LANES), f32),
            pltpu.VMEM((outer * each, LANES), f32),
            pltpu.VMEM((lags // LANES * each, LANES), f32),
            pltpu.SemaphoreType.DMA((len(loaded),)),
            *[pltpu.SemaphoreType.DMA((pairs,)) for _ in range(4)],
        ],
        compiler_params=pltpu.CompilerParams(collective_id=0, has_side_effects=True),
        name="detect",
    )(moveouts[None, :], traces, *loaded)


def solution(mesh):
    return jax.shard_map(
        functools.partial(on_device, mesh.shape["tm"]),
        mesh=mesh,
        in_specs=(P("grp", "tm"), P("tm", None), P("grp"), P(None, "grp")),
        out_specs=P("tm", "grp"),
        check_vma=False,
    )
```

```python
import functools
import math

import jax
import jax.numpy as jnp
import numpy as np
from jax import lax
from jax.experimental import pallas as pl
from jax.experimental.pallas import tpu as pltpu
from jax.sharding import PartitionSpec as P

f32, bf16 = jnp.float32, jnp.bfloat16
LANES = 128
REACH = 2048
COARSE = 4


def split(value):
    high = value.astype(bf16)
    return high, (value - high.astype(f32)).astype(bf16)


def split_table(table):
    high = table.astype(jnp.bfloat16)
    return high, (table - high.astype(np.float64)).astype(jnp.bfloat16)


def transform(rows, first_ref, forward_ref, cosine, sine):
    outer = cosine.shape[0]
    high, low = split(jnp.concatenate(rows, axis=1))
    first = jnp.dot(first_ref[...], jnp.concatenate([high, high, low], axis=0), preferred_element_type=f32)
    turned = []
    for r in range(len(rows)):
        re = first[:outer, r * LANES : (r + 1) * LANES]
        im = first[outer:, r * LANES : (r + 1) * LANES]
        turned.append(jnp.concatenate([re * cosine + im * sine, im * cosine - re * sine], axis=1))
    high, low = split(jnp.concatenate(turned, axis=0))
    return jnp.dot(jnp.concatenate([high, low, high], axis=1), forward_ref[...], preferred_element_type=f32)


def shift(traces_ref, late, terms, base, group, channels):
    rows = 16
    blocks = traces_ref.shape[1] // LANES
    here = pl.ds(pl.multiple_of(group * rows, rows), rows)
    delay = late[here, :]
    lane = lax.broadcasted_iota(jnp.int32, (rows, LANES), 1)
    inner = (delay & (LANES - 1)) + 1
    index = (lane - inner) & (LANES - 1)
    keep = lane >= inner
    turned = [
        jnp.take_along_axis(
            traces_ref[here, b * LANES : (b + 1) * LANES], index, axis=1, mode="promise_in_bounds"
        )
        for b in range(blocks)
    ]
    zero = jnp.zeros((rows, LANES), f32)
    moved = [
        jnp.where(keep, turned[b] if b < blocks else zero, turned[b - 1] if b > 0 else zero)
        for b in range(blocks + 1)
    ]
    hop = 1
    while hop < COARSE:
        chosen = ((delay // LANES) & hop) != 0
        moved = [
            jnp.where(
                chosen,
                moved[b - hop] if b >= hop else zero,
                moved[b] if b < len(moved) else zero,
            )
            for b in range(len(moved) + hop)
        ]
        hop *= 2
    for b in range(len(moved)):
        high, low = split(moved[b])
        column = slice(b * LANES, (b + 1) * LANES)
        terms[pl.ds(pl.multiple_of(base + group * rows, rows), rows), column] = high
        terms[pl.ds(pl.multiple_of(channels + base + group * rows, rows), rows), column] = low


def kernel(
    devices,
    channels,
    moveout_ref,
    moveouts_ref,
    traces_ref,
    mask_hbm,
    template_hbm,
    first_hbm,
    forward_hbm,
    back_hbm,
    last_hbm,
    twiddle_hbm,
    out_ref,
    mask_ref,
    template_ref,
    first_ref,
    forward_ref,
    back_ref,
    last_ref,
    twiddle_ref,
    late,
    terms,
    raw,
    part,
    arrived,
    merged,
    joined,
    series,
    tail,
    load_sem,
    pair_send,
    pair_recv,
    send_sem,
    recv_sem,
):
    step = pl.program_id(0)
    steps = pl.num_programs(0)
    depth, width = traces_ref.shape
    each, lags = template_ref.shape
    pairs = devices // 2
    me = lax.axis_index("tm")
    core = lax.rem(me, 2)
    pair = me // 2
    partner = me + 1 - 2 * core
    blocks = width // LANES
    window = blocks + REACH // LANES
    outer = devices * blocks
    loads = [
        pltpu.make_async_copy(source, target, load_sem.at[i])
        for i, (source, target) in enumerate(
            (
                (mask_hbm, mask_ref),
                (template_hbm, template_ref),
                (first_hbm, first_ref),
                (forward_hbm, forward_ref),
                (twiddle_hbm, twiddle_ref),
                (back_hbm, back_ref),
                (last_hbm, last_ref),
            )
        )
    ]
    barrier = pltpu.get_barrier_semaphore()

    @pl.when(step == 0)
    def _():
        for load in loads:
            load.start()

        def greet(i, _):
            target = 2 * lax.rem(pair + i, pairs) + core
            pl.semaphore_signal(barrier, inc=1, device_id={"tm": target}, device_id_type=pl.DeviceIdType.MESH)
            return 0

        pl.semaphore_signal(barrier, inc=1, device_id={"tm": partner}, device_id_type=pl.DeviceIdType.MESH)
        lax.fori_loop(1, pairs, greet, 0)

    for piece in range(depth // LANES):
        row = (REACH - 1) - moveout_ref[:, piece * LANES : (piece + 1) * LANES]
        late[piece * LANES : (piece + 1) * LANES, :] = jnp.broadcast_to(row, (LANES, LANES)).T

    def four_groups(i, _):
        for k in range(4):
            shift(traces_ref, late, terms, step * depth, 4 * i + k, channels)
        return 0

    lax.fori_loop(0, depth // 64, four_groups, 0)

    def far(k):
        near = (k + 1) // 2
        return lax.rem(pair + pairs // 2 + near * (1 - 2 * lax.rem(k, 2)), pairs)

    def to_partner(g):
        return pltpu.make_async_remote_copy(
            src_ref=part.at[1 - core, g],
            dst_ref=arrived.at[g],
            send_sem=pair_send.at[g],
            recv_sem=pair_recv.at[g],
            device_id={"tm": partner},
            device_id_type=pl.DeviceIdType.MESH,
        )

    def to_owner(k):
        g = far(k)
        return pltpu.make_async_remote_copy(
            src_ref=merged.at[g],
            dst_ref=joined.at[pair],
            send_sem=send_sem.at[k],
            recv_sem=recv_sem.at[k],
            device_id={"tm": 2 * g + core},
            device_id_type=pl.DeviceIdType.MESH,
        )

    @pl.when(step == steps - 1)
    def _():
        loads[0].wait()
        count = mask_ref.shape[0]
        coarse = ((REACH - 1) - moveouts_ref[...]) // (COARSE * LANES)
        chosen = [
            jnp.where(coarse == h, mask_ref[...], 0).astype(f32).astype(bf16)
            for h in range(REACH // LANES // COARSE)
        ]
        masks = jnp.concatenate(chosen, axis=0)
        double = jnp.concatenate([masks, masks], axis=1)
        fine = blocks + COARSE
        span = 2 if fine % 2 == 0 else 1
        for b in range(0, fine, span):
            column = slice(b * LANES, (b + span) * LANES)
            raw[:, column] = jnp.dot(double, terms[:, column], preferred_element_type=f32)

        def stacked(b):
            hops = [h for h in range(len(chosen)) if 0 <= b - COARSE * h < fine]
            return sum(
                raw[h * count : (h + 1) * count, (b - COARSE * h) * LANES : (b - COARSE * h + 1) * LANES]
                for h in hops
            )

        span = 2 if window % 2 == 0 else 1
        for b in range(0, window, span):
            added = [stacked(b + j) for j in range(span)]
            for owner in range(devices):
                part[owner % 2, owner // 2, b * each : (b + span) * each, :] = jnp.concatenate(
                    [value[owner * each : (owner + 1) * each] for value in added], axis=0
                )
        pl.semaphore_wait(barrier, pairs)

        def first_send(k, _):
            to_partner(far(k)).start()
            return 0

        lax.fori_loop(0, pairs - 1, first_send, 0)
        to_partner(pair).start()
        rows, more = window * each, blocks * each

        def merge(g):
            to_partner(g).wait_recv()
            own, other = part[core, g], arrived[g]
            early = jnp.where(core == 0, own, other)
            later = jnp.where(core == 0, other, own)
            middle = early[more:] + later[: rows - more]
            return early[:more], middle, later[rows - more :]

        def second_send(k, _):
            g = far(k)
            begin, middle, end = merge(g)
            merged[g, 0:more] = begin
            merged[g, more:rows] = middle
            merged[g, rows : rows + more] = end
            to_owner(k).start()
            return 0

        lax.fori_loop(0, pairs - 1, second_send, 0)
        begin, middle, end = merge(pair)
        joined[pair, 0:more] = begin
        joined[pair, more:rows] = middle
        joined[pair, rows : rows + more] = end

        for load in loads[1:]:
            load.wait()
        cosine, sine = twiddle_ref[0], twiddle_ref[1]
        values = template_ref[...]
        count = lags // LANES
        for b in range(count):
            series[b * each : (b + 1) * each, :] = values[:, b * LANES : (b + 1) * LANES]
        series[count * each :, :] = jnp.zeros(((outer - count) * each, LANES), f32)
        energy = jnp.sqrt(jnp.sum(values * values, axis=1, keepdims=True) + 1e-06)
        factor = 1.0 / (outer * LANES * math.sqrt(channels) * energy)

        def columns():
            return [series[pl.ds(k, outer, stride=each), :] for k in range(each)]

        templ = transform(columns(), first_ref, forward_ref, cosine, sine)

        def finish(k, _):
            to_owner(k).wait()
            return 0

        lax.fori_loop(0, pairs - 1, finish, 0)

        def leave(g, _):
            to_partner(g).wait_send()
            return 0

        lax.fori_loop(0, pairs, leave, 0)
        series[...] = jnp.zeros(series.shape, f32)
        local = 2 * blocks
        wide = window + blocks
        for source in range(pairs):
            for b in range(0, wide, local):
                taken = min(local, wide - b)
                block = (source * local + b - REACH // LANES) % outer
                here = slice(block * each, (block + taken) * each)
                series[here, :] = series[here, :] + joined[source, b * each : (b + taken) * each, :]
        stack = transform(columns(), first_ref, forward_ref, cosine, sine)
        stack_re, stack_im = stack[:, :LANES], stack[:, LANES:]
        templ_re, templ_im = templ[:, :LANES], templ[:, LANES:]
        product = jnp.concatenate(
            [stack_re * templ_re + stack_im * templ_im, stack_im * templ_re - stack_re * templ_im], axis=1
        )
        high, low = split(product)
        back = jnp.dot(jnp.concatenate([high, low, high], axis=1), back_ref[...], preferred_element_type=f32)
        turned = []
        for k in range(each):
            re = back[k * outer : (k + 1) * outer, :LANES]
            im = back[k * outer : (k + 1) * outer, LANES:]
            turned.append(jnp.concatenate([re * cosine - im * sine, re * sine + im * cosine], axis=0))
        high, low = split(jnp.concatenate(turned, axis=1))
        final = jnp.dot(last_ref[...], jnp.concatenate([high, high, low], axis=0), preferred_element_type=f32)
        for k in range(each):
            tail[pl.ds(k, count, stride=each), :] = final[:, k * LANES : (k + 1) * LANES]
        for b in range(count):
            out_ref[:, b * LANES : (b + 1) * LANES] = tail[b * each : (b + 1) * each, :] * factor


def tables(length, lags):
    outer = length // LANES
    turn = 2.0 * math.pi
    ramp = np.arange(outer)[:, None] * np.arange(outer)[None, :] % outer * (turn / outer)
    wide = np.arange(LANES)[:, None] * np.arange(LANES)[None, :] % LANES * (turn / LANES)
    twist = np.arange(outer)[:, None] * np.arange(LANES)[None, :] % length * (turn / length)
    first = split_table(np.concatenate([np.cos(ramp), -np.sin(ramp)], axis=0))
    cosine, sine = np.cos(wide), np.sin(wide)
    forward = split_table(np.block([[cosine, -sine], [sine, cosine]]))
    back = split_table(np.block([[cosine, sine], [-sine, cosine]]))
    shown = ramp[: lags // LANES]
    last = split_table(np.concatenate([np.cos(shown), -np.sin(shown)], axis=1))
    return (
        np.concatenate([first[0], first[1], first[0]], axis=1),
        np.concatenate([forward[0], forward[0], forward[1]], axis=0),
        np.concatenate([back[0], back[0], back[1]], axis=0),
        np.concatenate([last[0], last[1], last[0]], axis=1),
        np.stack([np.cos(twist), np.sin(twist)]).astype(np.float32),
    )


def on_device(devices, traces, templates, moveouts, masks):
    channels, width = traces.shape
    each, lags = templates.shape
    blocks = width // LANES
    outer = devices * blocks
    window = blocks + REACH // LANES
    depth = math.gcd(channels, 256)
    pairs = devices // 2
    loaded = [masks, templates, *[jnp.asarray(table) for table in tables(outer * LANES, lags)]]
    wide = (window + blocks) * each
    return pl.pallas_call(
        functools.partial(kernel, devices, channels),
        grid=(channels // depth,),
        in_specs=[
            pl.BlockSpec((1, depth), lambda i: (0, i)),
            pl.BlockSpec((1, channels), lambda i: (0, 0)),
            pl.BlockSpec((depth, width), lambda i: (i, 0)),
            *[pl.BlockSpec(memory_space=pl.ANY) for _ in loaded],
        ],
        out_specs=pl.BlockSpec((each, lags), lambda i: (0, 0)),
        out_shape=jax.ShapeDtypeStruct((each, lags), f32),
        scratch_shapes=[
            *[pltpu.VMEM(value.shape, value.dtype) for value in loaded],
            pltpu.VMEM((depth, LANES), jnp.int32),
            pltpu.VMEM((2 * channels, (blocks + COARSE) * LANES), bf16),
            pltpu.VMEM((REACH // LANES // COARSE * masks.shape[0], (blocks + COARSE) * LANES), f32),
            pltpu.VMEM((2, pairs, window * each, LANES), f32),
            pltpu.VMEM((pairs, window * each, LANES), f32),
            pltpu.VMEM((pairs, wide, LANES), f32),
            pltpu.VMEM((pairs, wide, LANES), f32),
            pltpu.VMEM((outer * each, LANES), f32),
            pltpu.VMEM((lags // LANES * each, LANES), f32),
            pltpu.SemaphoreType.DMA((len(loaded),)),
            *[pltpu.SemaphoreType.DMA((pairs,)) for _ in range(4)],
        ],
        compiler_params=pltpu.CompilerParams(collective_id=0, has_side_effects=True),
        name="detect",
    )(moveouts[None, :], moveouts[None, :], traces, *loaded)


def solution(mesh):
    return jax.shard_map(
        functools.partial(on_device, mesh.shape["tm"]),
        mesh=mesh,
        in_specs=(P("grp", "tm"), P("tm", None), P("grp"), P(None, "grp")),
        out_specs=P("tm", "grp"),
        check_vma=False,
    )
```

```python
import functools
import math

import jax
import jax.numpy as jnp
import numpy as np
from jax import lax
from jax.experimental import pallas as pl
from jax.experimental.pallas import tpu as pltpu
from jax.sharding import PartitionSpec as P

f32, bf16 = jnp.float32, jnp.bfloat16
LANES = 128
REACH = 2048
COARSE = 4


def split(value):
    high = value.astype(bf16)
    return high, (value - high.astype(f32)).astype(bf16)


def split_table(table):
    high = table.astype(jnp.bfloat16)
    return high, (table - high.astype(np.float64)).astype(jnp.bfloat16)


def transform(rows, first_ref, forward_ref, cosine, sine):
    outer = cosine.shape[0]
    high, low = split(jnp.concatenate(rows, axis=1))
    first = jnp.dot(first_ref[...], jnp.concatenate([high, high, low], axis=0), preferred_element_type=f32)
    turned = []
    for r in range(len(rows)):
        re = first[:outer, r * LANES : (r + 1) * LANES]
        im = first[outer:, r * LANES : (r + 1) * LANES]
        turned.append(jnp.concatenate([re * cosine + im * sine, im * cosine - re * sine], axis=1))
    high, low = split(jnp.concatenate(turned, axis=0))
    return jnp.dot(jnp.concatenate([high, low, high], axis=1), forward_ref[...], preferred_element_type=f32)


def shift(traces_ref, late, terms, base, group, channels):
    rows = 16
    blocks = traces_ref.shape[1] // LANES
    here = pl.ds(pl.multiple_of(group * rows, rows), rows)
    delay = late[here, :]
    lane = lax.broadcasted_iota(jnp.int32, (rows, LANES), 1)
    inner = (delay & (LANES - 1)) + 1
    index = (lane - inner) & (LANES - 1)
    keep = lane >= inner
    turned = [
        jnp.take_along_axis(
            traces_ref[here, b * LANES : (b + 1) * LANES], index, axis=1, mode="promise_in_bounds"
        )
        for b in range(blocks)
    ]
    zero = jnp.zeros((rows, LANES), f32)
    moved = [
        jnp.where(keep, turned[b] if b < blocks else zero, turned[b - 1] if b > 0 else zero)
        for b in range(blocks + 1)
    ]
    hop = 1
    while hop < COARSE:
        chosen = ((delay // LANES) & hop) != 0
        moved = [
            jnp.where(
                chosen,
                moved[b - hop] if b >= hop else zero,
                moved[b] if b < len(moved) else zero,
            )
            for b in range(len(moved) + hop)
        ]
        hop *= 2
    for b in range(len(moved)):
        high, low = split(moved[b])
        column = slice(b * LANES, (b + 1) * LANES)
        terms[pl.ds(pl.multiple_of(base + group * rows, rows), rows), column] = high
        terms[pl.ds(pl.multiple_of(channels + base + group * rows, rows), rows), column] = low


def kernel(
    devices,
    channels,
    moveout_ref,
    moveouts_ref,
    traces_ref,
    mask_hbm,
    template_hbm,
    first_hbm,
    forward_hbm,
    back_hbm,
    last_hbm,
    twiddle_hbm,
    out_ref,
    mask_ref,
    template_ref,
    first_ref,
    forward_ref,
    back_ref,
    last_ref,
    twiddle_ref,
    late,
    terms,
    raw,
    part,
    arrived,
    merged,
    joined,
    series,
    tail,
    load_sem,
    pair_send,
    pair_recv,
    send_sem,
    recv_sem,
):
    step = pl.program_id(0)
    steps = pl.num_programs(0)
    depth, width = traces_ref.shape
    each, lags = template_ref.shape
    pairs = devices // 2
    me = lax.axis_index("tm")
    core = lax.rem(me, 2)
    pair = me // 2
    partner = me + 1 - 2 * core
    blocks = width // LANES
    window = blocks + REACH // LANES
    outer = devices * blocks
    loads = [
        pltpu.make_async_copy(source, target, load_sem.at[i])
        for i, (source, target) in enumerate(
            (
                (mask_hbm, mask_ref),
                (template_hbm, template_ref),
                (first_hbm, first_ref),
                (forward_hbm, forward_ref),
                (twiddle_hbm, twiddle_ref),
                (back_hbm, back_ref),
                (last_hbm, last_ref),
            )
        )
    ]
    barrier = pltpu.get_barrier_semaphore()

    @pl.when(step == 0)
    def _():
        for load in loads:
            load.start()

        def greet(i, _):
            target = 2 * lax.rem(pair + i, pairs) + core
            pl.semaphore_signal(barrier, inc=1, device_id={"tm": target}, device_id_type=pl.DeviceIdType.MESH)
            return 0

        pl.semaphore_signal(barrier, inc=1, device_id={"tm": partner}, device_id_type=pl.DeviceIdType.MESH)
        lax.fori_loop(1, pairs, greet, 0)

    for piece in range(depth // LANES):
        row = (REACH - 1) - moveout_ref[:, piece * LANES : (piece + 1) * LANES]
        late[piece * LANES : (piece + 1) * LANES, :] = jnp.broadcast_to(row, (LANES, LANES)).T

    def four_groups(i, _):
        for k in range(4):
            shift(traces_ref, late, terms, step * depth, 4 * i + k, channels)
        return 0

    lax.fori_loop(0, depth // 64, four_groups, 0)

    middle_of = pairs // 2
    own_half = pair // middle_of

    def peer(stage, j):
        half = own_half if stage else 1 - own_half
        return half * middle_of + lax.rem(pair + j, middle_of)

    def to_partner(g):
        return pltpu.make_async_remote_copy(
            src_ref=part.at[1 - core, g],
            dst_ref=arrived.at[g],
            send_sem=pair_send.at[g],
            recv_sem=pair_recv.at[g],
            device_id={"tm": partner},
            device_id_type=pl.DeviceIdType.MESH,
        )

    def to_owner(stage, j):
        g = peer(stage, j)
        k = j + stage * (middle_of - 1)
        return pltpu.make_async_remote_copy(
            src_ref=merged.at[g],
            dst_ref=joined.at[pair],
            send_sem=send_sem.at[k],
            recv_sem=recv_sem.at[k],
            device_id={"tm": 2 * g + core},
            device_id_type=pl.DeviceIdType.MESH,
        )

    @pl.when(step == steps - 1)
    def _():
        loads[0].wait()
        count = mask_ref.shape[0] // 2
        coarse = ((REACH - 1) - moveouts_ref[...]) // (COARSE * LANES)
        hops = REACH // LANES // COARSE
        fine = blocks + COARSE

        def stacks(half):
            held = mask_ref[pl.ds(pl.multiple_of(half * count, 8), count), :]
            chosen = [jnp.where(coarse == h, held, 0).astype(f32).astype(bf16) for h in range(hops)]
            masks = jnp.concatenate(chosen, axis=0)
            double = jnp.concatenate([masks, masks], axis=1)
            span = 2 if fine % 2 == 0 else 1
            for b in range(0, fine, span):
                column = slice(b * LANES, (b + span) * LANES)
                raw[:, column] = jnp.dot(double, terms[:, column], preferred_element_type=f32)

            def stacked(b):
                return sum(
                    raw[h * count : (h + 1) * count, (b - COARSE * h) * LANES : (b - COARSE * h + 1) * LANES]
                    for h in range(hops)
                    if 0 <= b - COARSE * h < fine
                )

            span = 2 if window % 2 == 0 else 1
            for b in range(0, window, span):
                added = [stacked(b + j) for j in range(span)]
                for owner in range(pairs):
                    part[owner % 2, half * middle_of + owner // 2, b * each : (b + span) * each, :] = (
                        jnp.concatenate([value[owner * each : (owner + 1) * each] for value in added], axis=0)
                    )

        def first_sends(stage):
            def start(j, _):
                to_partner(peer(stage, j)).start()
                return 0

            lax.fori_loop(stage, middle_of, start, 0)

        stacks(1 - own_half)
        pl.semaphore_wait(barrier, pairs)
        first_sends(0)
        stacks(own_half)
        first_sends(1)
        to_partner(pair).start()
        rows, more = window * each, blocks * each

        def merge(g):
            to_partner(g).wait_recv()
            own, other = part[core, g], arrived[g]
            early = jnp.where(core == 0, own, other)
            later = jnp.where(core == 0, other, own)
            middle = early[more:] + later[: rows - more]
            return early[:more], middle, later[rows - more :]

        def second_sends(stage):
            def start(j, _):
                g = peer(stage, j)
                begin, middle, end = merge(g)
                merged[g, 0:more] = begin
                merged[g, more:rows] = middle
                merged[g, rows : rows + more] = end
                to_owner(stage, j).start()
                return 0

            lax.fori_loop(stage, middle_of, start, 0)

        second_sends(0)
        second_sends(1)
        begin, middle, end = merge(pair)
        joined[pair, 0:more] = begin
        joined[pair, more:rows] = middle
        joined[pair, rows : rows + more] = end

        for load in loads[1:]:
            load.wait()
        cosine, sine = twiddle_ref[0], twiddle_ref[1]
        values = template_ref[...]
        count = lags // LANES
        for b in range(count):
            series[b * each : (b + 1) * each, :] = values[:, b * LANES : (b + 1) * LANES]
        series[count * each :, :] = jnp.zeros(((outer - count) * each, LANES), f32)
        energy = jnp.sqrt(jnp.sum(values * values, axis=1, keepdims=True) + 1e-06)
        factor = 1.0 / (outer * LANES * math.sqrt(channels) * energy)

        def columns():
            return [series[pl.ds(k, outer, stride=each), :] for k in range(each)]

        templ = transform(columns(), first_ref, forward_ref, cosine, sine)

        def finish(stage):
            def wait(j, _):
                to_owner(stage, j).wait()
                return 0

            lax.fori_loop(stage, middle_of, wait, 0)

        finish(1)
        finish(0)

        def leave(g, _):
            to_partner(g).wait_send()
            return 0

        lax.fori_loop(0, pairs, leave, 0)
        series[...] = jnp.zeros(series.shape, f32)
        local = 2 * blocks
        wide = window + blocks
        for source in range(pairs):
            for b in range(0, wide, local):
                taken = min(local, wide - b)
                block = (source * local + b - REACH // LANES) % outer
                here = slice(block * each, (block + taken) * each)
                series[here, :] = series[here, :] + joined[source, b * each : (b + taken) * each, :]
        stack = transform(columns(), first_ref, forward_ref, cosine, sine)
        stack_re, stack_im = stack[:, :LANES], stack[:, LANES:]
        templ_re, templ_im = templ[:, :LANES], templ[:, LANES:]
        product = jnp.concatenate(
            [stack_re * templ_re + stack_im * templ_im, stack_im * templ_re - stack_re * templ_im], axis=1
        )
        high, low = split(product)
        back = jnp.dot(jnp.concatenate([high, low, high], axis=1), back_ref[...], preferred_element_type=f32)
        turned = []
        for k in range(each):
            re = back[k * outer : (k + 1) * outer, :LANES]
            im = back[k * outer : (k + 1) * outer, LANES:]
            turned.append(jnp.concatenate([re * cosine - im * sine, re * sine + im * cosine], axis=0))
        high, low = split(jnp.concatenate(turned, axis=1))
        final = jnp.dot(last_ref[...], jnp.concatenate([high, high, low], axis=0), preferred_element_type=f32)
        for k in range(each):
            tail[pl.ds(k, count, stride=each), :] = final[:, k * LANES : (k + 1) * LANES]
        for b in range(count):
            out_ref[:, b * LANES : (b + 1) * LANES] = tail[b * each : (b + 1) * each, :] * factor


def tables(length, lags):
    outer = length // LANES
    turn = 2.0 * math.pi
    ramp = np.arange(outer)[:, None] * np.arange(outer)[None, :] % outer * (turn / outer)
    wide = np.arange(LANES)[:, None] * np.arange(LANES)[None, :] % LANES * (turn / LANES)
    twist = np.arange(outer)[:, None] * np.arange(LANES)[None, :] % length * (turn / length)
    first = split_table(np.concatenate([np.cos(ramp), -np.sin(ramp)], axis=0))
    cosine, sine = np.cos(wide), np.sin(wide)
    forward = split_table(np.block([[cosine, -sine], [sine, cosine]]))
    back = split_table(np.block([[cosine, sine], [-sine, cosine]]))
    shown = ramp[: lags // LANES]
    last = split_table(np.concatenate([np.cos(shown), -np.sin(shown)], axis=1))
    return (
        np.concatenate([first[0], first[1], first[0]], axis=1),
        np.concatenate([forward[0], forward[0], forward[1]], axis=0),
        np.concatenate([back[0], back[0], back[1]], axis=0),
        np.concatenate([last[0], last[1], last[0]], axis=1),
        np.stack([np.cos(twist), np.sin(twist)]).astype(np.float32),
    )


def on_device(devices, traces, templates, moveouts, masks):
    channels, width = traces.shape
    each, lags = templates.shape
    blocks = width // LANES
    outer = devices * blocks
    window = blocks + REACH // LANES
    depth = math.gcd(channels, 256)
    pairs = devices // 2
    loaded = [masks, templates, *[jnp.asarray(table) for table in tables(outer * LANES, lags)]]
    wide = (window + blocks) * each
    return pl.pallas_call(
        functools.partial(kernel, devices, channels),
        grid=(channels // depth,),
        in_specs=[
            pl.BlockSpec((1, depth), lambda i: (0, i)),
            pl.BlockSpec((1, channels), lambda i: (0, 0)),
            pl.BlockSpec((depth, width), lambda i: (i, 0)),
            *[pl.BlockSpec(memory_space=pl.ANY) for _ in loaded],
        ],
        out_specs=pl.BlockSpec((each, lags), lambda i: (0, 0)),
        out_shape=jax.ShapeDtypeStruct((each, lags), f32),
        scratch_shapes=[
            *[pltpu.VMEM(value.shape, value.dtype) for value in loaded],
            pltpu.VMEM((depth, LANES), jnp.int32),
            pltpu.VMEM((2 * channels, (blocks + COARSE) * LANES), bf16),
            pltpu.VMEM((REACH // LANES // COARSE * masks.shape[0] // 2, (blocks + COARSE) * LANES), f32),
            pltpu.VMEM((2, pairs, window * each, LANES), f32),
            pltpu.VMEM((pairs, window * each, LANES), f32),
            pltpu.VMEM((pairs, wide, LANES), f32),
            pltpu.VMEM((pairs, wide, LANES), f32),
            pltpu.VMEM((outer * each, LANES), f32),
            pltpu.VMEM((lags // LANES * each, LANES), f32),
            pltpu.SemaphoreType.DMA((len(loaded),)),
            *[pltpu.SemaphoreType.DMA((pairs,)) for _ in range(4)],
        ],
        compiler_params=pltpu.CompilerParams(collective_id=0, has_side_effects=True),
        name="detect",
    )(moveouts[None, :], moveouts[None, :], traces, *loaded)


def solution(mesh):
    return jax.shard_map(
        functools.partial(on_device, mesh.shape["tm"]),
        mesh=mesh,
        in_specs=(P("grp", "tm"), P("tm", None), P("grp"), P(None, "grp")),
        out_specs=P("tm", "grp"),
        check_vma=False,
    )
```

```python
import functools
import math

import jax
import jax.numpy as jnp
import numpy as np
from jax import lax
from jax.experimental import pallas as pl
from jax.experimental.pallas import tpu as pltpu
from jax.sharding import PartitionSpec as P

f32, bf16 = jnp.float32, jnp.bfloat16
LANES = 128
REACH = 2048
COARSE = 4


def split(value):
    high = value.astype(bf16)
    return high, (value - high.astype(f32)).astype(bf16)


def split_table(table):
    high = table.astype(jnp.bfloat16)
    return high, (table - high.astype(np.float64)).astype(jnp.bfloat16)


def transform(rows, first_ref, forward_ref, cosine, sine):
    outer = cosine.shape[0]
    high, low = split(jnp.concatenate(rows, axis=1))
    first = jnp.dot(first_ref[...], jnp.concatenate([high, high, low], axis=0), preferred_element_type=f32)
    turned = []
    for r in range(len(rows)):
        re = first[:outer, r * LANES : (r + 1) * LANES]
        im = first[outer:, r * LANES : (r + 1) * LANES]
        turned.append(jnp.concatenate([re * cosine + im * sine, im * cosine - re * sine], axis=1))
    high, low = split(jnp.concatenate(turned, axis=0))
    return jnp.dot(jnp.concatenate([high, low, high], axis=1), forward_ref[...], preferred_element_type=f32)


def shift(traces_ref, late, terms, base, group, channels):
    rows = 16
    blocks = traces_ref.shape[1] // LANES
    here = pl.ds(pl.multiple_of(group * rows, rows), rows)
    delay = late[here, :]
    lane = lax.broadcasted_iota(jnp.int32, (rows, LANES), 1)
    inner = (delay & (LANES - 1)) + 1
    index = (lane - inner) & (LANES - 1)
    keep = lane >= inner
    turned = [
        jnp.take_along_axis(
            traces_ref[here, b * LANES : (b + 1) * LANES], index, axis=1, mode="promise_in_bounds"
        )
        for b in range(blocks)
    ]
    zero = jnp.zeros((rows, LANES), f32)
    moved = [
        jnp.where(keep, turned[b] if b < blocks else zero, turned[b - 1] if b > 0 else zero)
        for b in range(blocks + 1)
    ]
    hop = 1
    while hop < COARSE:
        chosen = ((delay // LANES) & hop) != 0
        moved = [
            jnp.where(
                chosen,
                moved[b - hop] if b >= hop else zero,
                moved[b] if b < len(moved) else zero,
            )
            for b in range(len(moved) + hop)
        ]
        hop *= 2
    for b in range(len(moved)):
        high, low = split(moved[b])
        column = slice(b * LANES, (b + 1) * LANES)
        terms[pl.ds(pl.multiple_of(base + group * rows, rows), rows), column] = high
        terms[pl.ds(pl.multiple_of(channels + base + group * rows, rows), rows), column] = low


def kernel(
    devices,
    channels,
    moveout_ref,
    moveouts_ref,
    traces_ref,
    mask_hbm,
    template_hbm,
    first_hbm,
    forward_hbm,
    back_hbm,
    last_hbm,
    twiddle_hbm,
    out_ref,
    mask_ref,
    template_ref,
    first_ref,
    forward_ref,
    back_ref,
    last_ref,
    twiddle_ref,
    late,
    terms,
    raw,
    part,
    arrived,
    merged,
    joined,
    series,
    tail,
    load_sem,
    pair_send,
    pair_recv,
    send_sem,
    recv_sem,
):
    step = pl.program_id(0)
    steps = pl.num_programs(0)
    depth, width = traces_ref.shape
    each, lags = template_ref.shape
    pairs = devices // 2
    me = lax.axis_index("tm")
    core = lax.rem(me, 2)
    pair = me // 2
    partner = me + 1 - 2 * core
    blocks = width // LANES
    window = blocks + REACH // LANES
    outer = devices * blocks
    loads = [
        pltpu.make_async_copy(source, target, load_sem.at[i])
        for i, (source, target) in enumerate(
            (
                (mask_hbm, mask_ref),
                (template_hbm, template_ref),
                (first_hbm, first_ref),
                (forward_hbm, forward_ref),
                (twiddle_hbm, twiddle_ref),
                (back_hbm, back_ref),
                (last_hbm, last_ref),
            )
        )
    ]
    barrier = pltpu.get_barrier_semaphore()

    @pl.when(step == 0)
    def _():
        for load in loads:
            load.start()

        def greet(i, _):
            target = 2 * lax.rem(pair + i, pairs) + core
            pl.semaphore_signal(barrier, inc=1, device_id={"tm": target}, device_id_type=pl.DeviceIdType.MESH)
            return 0

        pl.semaphore_signal(barrier, inc=1, device_id={"tm": partner}, device_id_type=pl.DeviceIdType.MESH)
        lax.fori_loop(1, pairs, greet, 0)

    for piece in range(depth // LANES):
        row = (REACH - 1) - moveout_ref[:, piece * LANES : (piece + 1) * LANES]
        late[piece * LANES : (piece + 1) * LANES, :] = jnp.broadcast_to(row, (LANES, LANES)).T

    def four_groups(i, _):
        for k in range(4):
            shift(traces_ref, late, terms, step * depth, 4 * i + k, channels)
        return 0

    lax.fori_loop(0, depth // 64, four_groups, 0)

    def peer(k):
        return lax.rem(pair + 1 + k, pairs)

    def to_partner(g):
        return pltpu.make_async_remote_copy(
            src_ref=part.at[1 - core, g],
            dst_ref=arrived.at[g],
            send_sem=pair_send.at[g],
            recv_sem=pair_recv.at[g],
            device_id={"tm": partner},
            device_id_type=pl.DeviceIdType.MESH,
        )

    def to_owner(k):
        g = peer(k)
        return pltpu.make_async_remote_copy(
            src_ref=merged.at[g],
            dst_ref=joined.at[pair],
            send_sem=send_sem.at[k],
            recv_sem=recv_sem.at[k],
            device_id={"tm": 2 * g + core},
            device_id_type=pl.DeviceIdType.MESH,
        )

    @pl.when(step == steps - 1)
    def _():
        loads[0].wait()
        count = mask_ref.shape[0]
        coarse = ((REACH - 1) - moveouts_ref[...]) // (COARSE * LANES)
        chosen = [
            jnp.where(coarse == h, mask_ref[...], 0).astype(f32).astype(bf16)
            for h in range(REACH // LANES // COARSE)
        ]
        masks = jnp.concatenate(chosen, axis=0)
        double = jnp.concatenate([masks, masks], axis=1)
        fine = blocks + COARSE
        span = 2 if fine % 2 == 0 else 1
        for b in range(0, fine, span):
            column = slice(b * LANES, (b + span) * LANES)
            raw[:, column] = jnp.dot(double, terms[:, column], preferred_element_type=f32)

        def stacked(b):
            hops = [h for h in range(len(chosen)) if 0 <= b - COARSE * h < fine]
            return sum(
                raw[h * count : (h + 1) * count, (b - COARSE * h) * LANES : (b - COARSE * h + 1) * LANES]
                for h in hops
            )

        span = 2 if window % 2 == 0 else 1
        for b in range(0, window, span):
            added = [stacked(b + j) for j in range(span)]
            for owner in range(devices):
                part[owner % 2, owner // 2, b * each : (b + span) * each, :] = jnp.concatenate(
                    [value[owner * each : (owner + 1) * each] for value in added], axis=0
                )
        pl.semaphore_wait(barrier, pairs)

        def first_send(k, _):
            to_partner(peer(k)).start()
            return 0

        lax.fori_loop(0, pairs - 1, first_send, 0)
        to_partner(pair).start()
        rows, more = window * each, blocks * each

        def merge(g):
            to_partner(g).wait_recv()
            own, other = part[core, g], arrived[g]
            early = jnp.where(core == 0, own, other)
            later = jnp.where(core == 0, other, own)
            middle = early[more:] + later[: rows - more]
            return early[:more], middle, later[rows - more :]

        def second_send(k, _):
            g = peer(k)
            begin, middle, end = merge(g)
            merged[g, 0:more] = begin
            merged[g, more:rows] = middle
            merged[g, rows : rows + more] = end
            to_owner(k).start()
            return 0

        lax.fori_loop(0, pairs - 1, second_send, 0)
        begin, middle, end = merge(pair)
        joined[pair, 0:more] = begin
        joined[pair, more:rows] = middle
        joined[pair, rows : rows + more] = end

        for load in loads[1:]:
            load.wait()
        cosine, sine = twiddle_ref[0], twiddle_ref[1]
        values = template_ref[...]
        count = lags // LANES
        for b in range(count):
            series[b * each : (b + 1) * each, :] = values[:, b * LANES : (b + 1) * LANES]
        series[count * each :, :] = jnp.zeros(((outer - count) * each, LANES), f32)
        energy = jnp.sqrt(jnp.sum(values * values, axis=1, keepdims=True) + 1e-06)
        factor = 1.0 / (outer * LANES * math.sqrt(channels) * energy)

        def columns():
            return [series[pl.ds(k, outer, stride=each), :] for k in range(each)]

        templ = transform(columns(), first_ref, forward_ref, cosine, sine)

        def finish(k, _):
            to_owner(k).wait()
            return 0

        lax.fori_loop(0, pairs - 1, finish, 0)

        def leave(g, _):
            to_partner(g).wait_send()
            return 0

        lax.fori_loop(0, pairs, leave, 0)
        series[...] = jnp.zeros(series.shape, f32)
        local = 2 * blocks
        wide = window + blocks
        for source in range(pairs):
            for b in range(0, wide, local):
                taken = min(local, wide - b)
                block = (source * local + b - REACH // LANES) % outer
                here = slice(block * each, (block + taken) * each)
                series[here, :] = series[here, :] + joined[source, b * each : (b + taken) * each, :]
        stack = transform(columns(), first_ref, forward_ref, cosine, sine)
        stack_re, stack_im = stack[:, :LANES], stack[:, LANES:]
        templ_re, templ_im = templ[:, :LANES], templ[:, LANES:]
        product = jnp.concatenate(
            [stack_re * templ_re + stack_im * templ_im, stack_im * templ_re - stack_re * templ_im], axis=1
        )
        high, low = split(product)
        back = jnp.dot(jnp.concatenate([high, low, high], axis=1), back_ref[...], preferred_element_type=f32)
        turned = []
        for k in range(each):
            re = back[k * outer : (k + 1) * outer, :LANES]
            im = back[k * outer : (k + 1) * outer, LANES:]
            turned.append(jnp.concatenate([re * cosine - im * sine, re * sine + im * cosine], axis=0))
        high, low = split(jnp.concatenate(turned, axis=1))
        final = jnp.dot(last_ref[...], jnp.concatenate([high, high, low], axis=0), preferred_element_type=f32)
        for k in range(each):
            tail[pl.ds(k, count, stride=each), :] = final[:, k * LANES : (k + 1) * LANES]
        for b in range(count):
            out_ref[:, b * LANES : (b + 1) * LANES] = tail[b * each : (b + 1) * each, :] * factor


def tables(length, lags):
    outer = length // LANES
    turn = 2.0 * math.pi
    ramp = np.arange(outer)[:, None] * np.arange(outer)[None, :] % outer * (turn / outer)
    wide = np.arange(LANES)[:, None] * np.arange(LANES)[None, :] % LANES * (turn / LANES)
    twist = np.arange(outer)[:, None] * np.arange(LANES)[None, :] % length * (turn / length)
    first = split_table(np.concatenate([np.cos(ramp), -np.sin(ramp)], axis=0))
    cosine, sine = np.cos(wide), np.sin(wide)
    forward = split_table(np.block([[cosine, -sine], [sine, cosine]]))
    back = split_table(np.block([[cosine, sine], [-sine, cosine]]))
    shown = ramp[: lags // LANES]
    last = split_table(np.concatenate([np.cos(shown), -np.sin(shown)], axis=1))
    return (
        np.concatenate([first[0], first[1], first[0]], axis=1),
        np.concatenate([forward[0], forward[0], forward[1]], axis=0),
        np.concatenate([back[0], back[0], back[1]], axis=0),
        np.concatenate([last[0], last[1], last[0]], axis=1),
        np.stack([np.cos(twist), np.sin(twist)]).astype(np.float32),
    )


def on_device(devices, traces, templates, moveouts, masks):
    channels, width = traces.shape
    each, lags = templates.shape
    blocks = width // LANES
    outer = devices * blocks
    window = blocks + REACH // LANES
    depth = math.gcd(channels, 256)
    pairs = devices // 2
    loaded = [masks, templates, *[jnp.asarray(table) for table in tables(outer * LANES, lags)]]
    wide = (window + blocks) * each
    return pl.pallas_call(
        functools.partial(kernel, devices, channels),
        grid=(channels // depth,),
        in_specs=[
            pl.BlockSpec((1, depth), lambda i: (0, i)),
            pl.BlockSpec((1, channels), lambda i: (0, 0)),
            pl.BlockSpec((depth, width), lambda i: (i, 0)),
            *[pl.BlockSpec(memory_space=pl.ANY) for _ in loaded],
        ],
        out_specs=pl.BlockSpec((each, lags), lambda i: (0, 0)),
        out_shape=jax.ShapeDtypeStruct((each, lags), f32),
        scratch_shapes=[
            *[pltpu.VMEM(value.shape, value.dtype) for value in loaded],
            pltpu.VMEM((depth, LANES), jnp.int32),
            pltpu.VMEM((2 * channels, (blocks + COARSE) * LANES), bf16),
            pltpu.VMEM((REACH // LANES // COARSE * masks.shape[0], (blocks + COARSE) * LANES), f32),
            pltpu.VMEM((2, pairs, window * each, LANES), f32),
            pltpu.VMEM((pairs, window * each, LANES), f32),
            pltpu.VMEM((pairs, wide, LANES), f32),
            pltpu.VMEM((pairs, wide, LANES), f32),
            pltpu.VMEM((outer * each, LANES), f32),
            pltpu.VMEM((lags // LANES * each, LANES), f32),
            pltpu.SemaphoreType.DMA((len(loaded),)),
            *[pltpu.SemaphoreType.DMA((pairs,)) for _ in range(4)],
        ],
        compiler_params=pltpu.CompilerParams(collective_id=0, has_side_effects=True),
        name="detect",
    )(moveouts[None, :], moveouts[None, :], traces, *loaded)


def solution(mesh):
    return jax.shard_map(
        functools.partial(on_device, mesh.shape["tm"]),
        mesh=mesh,
        in_specs=(P("grp", "tm"), P("tm", None), P("grp"), P(None, "grp")),
        out_specs=P("tm", "grp"),
        check_vma=False,
    )
```
